32 devices in a mesh: grid: 4 (over y, x), fsdp: 8 (over z, core).
Axes of the slice: x: 2, y: 2, z: 4, core: 2. Of those that a mesh axis runs over, the one named last changes fastest.
Arguments:
- hidden: bfloat16 [512, 4096], P('fsdp'), may hold values from -16 to 16
- norm_gain: float32 [4096], replicated, may hold values from 0.5 to 1.5
- base_head: bfloat16 [8192, 4096], P('fsdp'), may hold values from -1 to 1
- first_dir: bfloat16 [8192, 4096], P('fsdp'), may hold values from -0.09375 to 0.09375
- second_dir: bfloat16 [8192, 4096], P('fsdp'), may hold values from -0.09375 to 0.09375
- coords: int32 [8, 2], P('grid'), parts along dimension 0, may hold values from 0 to 7
- targets: int32 [512], replicated, may hold values from 0 to 8191
Outputs:
- token_loss: float32 [8, 512], P('grid', 'fsdp'), parts along dimension 0
- mean_loss: float32 [8], P('grid'), parts along dimension 0
The draws below stay inside these ranges and needn't reach their ends.
There are 4 independent parts, one for each index of `grid`. The reference program is written for one: setup_inputs(seed, part) draws one part's arguments, and reference() takes and returns one part's arrays. A program takes and returns all parts, laid end to end along the dimension named above; an argument that names none is the same for every part. Nothing has to cross between parts.
All inputs are finite; a program needn't handle non-finite values.
Results may differ from the reference program's by a relative error of at most 0.0003.
Values may be sent and summed in bfloat16 or wider, within the bound.
A program may use at most 128 MiB of HBM per device.

```python
import math
import jax
import jax.numpy as jnp
from jax import lax

D = 4096
V_DEV = 1024
PTS = 2
TOKENS = 512
VOCAB = 8192
N_FSDP = 8


def spike_plan(key):
    spike_key = jax.random.fold_in(key, 7177)
    spike_rows = jax.random.randint(jax.random.fold_in(spike_key, 1), (N_FSDP,), 0, TOKENS)
    offsets = jax.random.randint(jax.random.fold_in(spike_key, 2), (N_FSDP,), 0, V_DEV)
    spike_cols = jnp.arange(N_FSDP, dtype=jnp.int32) * V_DEV + offsets
    pattern = jnp.clip(jax.random.normal(jax.random.fold_in(spike_key, 3), (N_FSDP, D), jnp.float32), -3.0, 3.0)
    return (spike_rows, spike_cols, pattern)


def draw_hidden(key, part):
    rows_all = jnp.clip(jax.random.normal(jax.random.fold_in(key, 21), (TOKENS, D), jnp.float32), -4.0, 4.0)
    spike_rows, spike_cols, pattern = spike_plan(key)
    rows_all = rows_all.at[spike_rows].set(pattern)
    return rows_all.astype(jnp.bfloat16)


def draw_base_head(key, part):
    weight = jnp.clip(jax.random.normal(jax.random.fold_in(key, 11), (VOCAB, D), jnp.float32) / math.sqrt(D), -0.25, 0.25)
    spike_rows, spike_cols, pattern = spike_plan(key)
    weight = weight.at[spike_cols].set(240.0 / D * pattern)
    return weight.astype(jnp.bfloat16)


def touch_ends(result, key, low, high):
    longest = result.shape.index(max(result.shape))
    spots = []
    for shift in (0, 1):
        where = [jax.random.randint(jax.random.fold_in(key, axis), (), 0, length) for axis, length in enumerate(result.shape)]
        where[longest] = (where[longest] + shift) % result.shape[longest]
        spots.append(tuple(where))
    return result.at[spots[0]].set(low).at[spots[1]].set(high)


def block_levels(own_key, shape, pieces, low, top_value):
    loudness = 1.0
    for dim, blocks in pieces:
        draws = jax.random.uniform(jax.random.fold_in(jax.random.fold_in(own_key, 6), dim), (blocks,), jnp.float32, low / len(pieces), top_value / len(pieces))
        loudness = loudness * jnp.repeat(jnp.exp(draws), shape[dim] // blocks).reshape((-1,) + (1,) * (len(shape) - 1 - dim))
    return loudness


def bell_draw(own_key, extent, spread, bound, cuts=(), kind=jnp.bfloat16):
    entries = spread * jax.random.normal(own_key, extent, jnp.float32)
    if cuts:
        entries = entries * block_levels(own_key, extent, cuts, -0.22, 0.18)
    return jnp.clip(entries, -bound, bound).astype(kind)


def setup_inputs(seed: int = 0, part: int = 0) -> dict:
    keys = jax.random.split(jax.random.key(seed), 8)
    own_keys = jax.random.split(jax.random.fold_in(keys[7], part), 8)
    hidden = draw_hidden(jax.random.fold_in(keys[7], 71), part)
    norm_gain = jnp.clip(1.0 + 0.1 * jax.random.normal(keys[1], (D,), jnp.float32), 0.5, 1.5)
    base_head = draw_base_head(jax.random.fold_in(keys[7], 71), part)
    first_dir = bell_draw(keys[3], (VOCAB, D), D ** -0.5, 0.09375, ((0, 8),))
    second_dir = bell_draw(keys[4], (VOCAB, D), D ** -0.5, 0.09375, ((0, 8),))
    coords = touch_ends(jax.random.randint(own_keys[5], (PTS, 2), 0, 8), jax.random.fold_in(own_keys[5], 1), 0, 7).astype(jnp.int32)
    targets = touch_ends(jax.random.randint(keys[6], (TOKENS,), 0, VOCAB), jax.random.fold_in(keys[6], 1), 0, VOCAB - 1).astype(jnp.int32)
    return dict(hidden=hidden, norm_gain=norm_gain, base_head=base_head, first_dir=first_dir, second_dir=second_dir, coords=coords, targets=targets)


epsilon = 1e-05

def reference(hidden, norm_gain, base_head, first_dir, second_dir, coords, targets):
    level_table = (2.0 * jnp.arange(8, dtype=jnp.float32) - 7.0) / 7.0
    mixing = level_table[coords]
    widened = hidden.astype(jnp.float32)
    inv_rms = lax.rsqrt(lax.optimization_barrier(jnp.mean(widened * widened, axis=1, keepdims=True)) + epsilon)
    normed = (widened * inv_rms * norm_gain).astype(jnp.bfloat16)
    losses = []
    for point_idx in range(PTS):
        head_now = (base_head.astype(jnp.float32) + mixing[point_idx, 0] * first_dir.astype(jnp.float32) + mixing[point_idx, 1] * second_dir.astype(jnp.float32)).astype(jnp.bfloat16)
        logits = jnp.dot(normed, head_now.T, preferred_element_type=jnp.float32)
        row_top = lax.optimization_barrier(jnp.max(logits, axis=1, keepdims=True))
        log_total = row_top[:, 0] + jnp.log(lax.optimization_barrier(jnp.sum(jnp.exp(logits - row_top), axis=1)))
        picked = jnp.take_along_axis(logits, targets[:, None].astype(jnp.int32), axis=1)[:, 0]
        losses.append(log_total - picked)
    token_loss = jnp.stack(losses)
    return (token_loss, lax.optimization_barrier(jnp.mean(token_loss, axis=1)))
```

```python
import functools

import jax
import jax.numpy as jnp
from jax import lax
from jax.experimental import pallas as pl
from jax.experimental.pallas import tpu as pltpu
from jax.sharding import PartitionSpec as P

epsilon = 1e-05
MESH = pl.DeviceIdType.MESH
NUM_PIECES = 8
ROW_CHUNK = 32
LOG2E = 1.4426950408889634
LN2 = 0.6931471805599453


def kernel(
    n_grid, n_fsdp, total_tokens,
    coords_hbm, hidden_hbm, gain_hbm, targets_hbm, base_hbm, first_hbm, second_hbm,
    packed_ref,
    coords_ref, hidden_ref, gain_ref, targets_ref,
    w_buf, x_buf, acc, mix_own, mix_all, stat_own, stat_all,
    small_sem, w_sem, chain_send, chain_recv, pair_send, pair_recv,
    mix_send, mix_recv, stat_send, stat_recv, known_sem,
):
    g = lax.axis_index("grid")
    f = lax.axis_index("fsdp")
    nz = n_fsdp // 2
    z, core = f // 2, f % 2
    n_all = n_grid * n_fsdp
    me = g * n_fsdp + f
    pts = coords_hbm.shape[0]
    chunk, width = hidden_ref.shape
    vocab = base_hbm.shape[0]
    kp = x_buf.shape[4]
    lanes = 2 * nz * chunk
    last = nz - 1
    is_end = jnp.logical_or(z == 0, z == last)

    barrier = pltpu.get_barrier_semaphore()
    for d in range(1, n_fsdp):
        pl.semaphore_signal(
            barrier, inc=1, device_id=(g, lax.rem(f + d, n_fsdp)), device_id_type=MESH
        )
    for d in range(1, n_grid):
        pl.semaphore_signal(
            barrier, inc=1, device_id=(lax.rem(g + d, n_grid), f), device_id_type=MESH
        )

    rows = pl.ds(pl.multiple_of(g * chunk, chunk), chunk)
    small = [
        pltpu.make_async_copy(hidden_hbm.at[rows, :], hidden_ref, small_sem.at[0]),
        pltpu.make_async_copy(gain_hbm, gain_ref, small_sem.at[1]),
        pltpu.make_async_copy(coords_hbm, coords_ref, small_sem.at[2]),
        pltpu.make_async_copy(targets_hbm, targets_ref, small_sem.at[3]),
    ]
    for copy in small:
        copy.start()

    @pl.loop(0, NUM_PIECES)
    def _(p):
        cols = pl.ds(pl.multiple_of(p * kp, kp), kp)
        for j, src in enumerate((base_hbm, first_hbm, second_hbm)):
            pltpu.make_async_copy(src.at[:, cols], w_buf.at[p, j], w_sem.at[p]).start()

    small[0].wait()
    small[1].wait()
    squares = jnp.zeros((chunk, 1), jnp.float32)
    for p in range(NUM_PIECES):
        wide = hidden_ref[:, p * kp : (p + 1) * kp].astype(jnp.float32)
        squares = squares + jnp.sum(wide * wide, axis=1, keepdims=True)
    inv_rms = lax.rsqrt(squares / width + epsilon)
    for p in range(NUM_PIECES):
        wide = hidden_ref[:, p * kp : (p + 1) * kp].astype(jnp.float32)
        gain = gain_ref[:, p * kp : (p + 1) * kp]
        x_buf[p, pl.ds(core, 1), pl.ds(z, 1)] = (
            (wide * inv_rms * gain).astype(jnp.bfloat16)[None, None]
        )

    pl.semaphore_wait(barrier, n_fsdp + n_grid - 2)

    def chain_copy(p, s, target):
        return pltpu.make_async_remote_copy(
            src_ref=x_buf.at[p, core, s], dst_ref=x_buf.at[p, core, s],
            send_sem=chain_send, recv_sem=chain_recv.at[p, s],
            device_id=(g, 2 * target + core), device_id_type=MESH,
        )

    def pair_copy(p, s):
        return pltpu.make_async_remote_copy(
            src_ref=x_buf.at[p, core, s], dst_ref=x_buf.at[p, core, s],
            send_sem=pair_send, recv_sem=pair_recv.at[p],
            device_id=(g, f + 1 - 2 * core), device_id_type=MESH,
        )

    @pl.loop(0, NUM_PIECES)
    def _(p):
        @pl.when(is_end)
        def _():
            for i in range(last):
                chain_copy(p, z, jnp.where(z == 0, last - i, i)).start()

        @pl.when(jnp.logical_not(is_end))
        def _():
            chain_copy(p, z, z + 1).start()
            chain_copy(p, z, z - 1).start()

        pair_copy(p, z).start()

    small[2].wait()
    for pt in range(pts):
        for k in range(2):
            level = jnp.broadcast_to(coords_ref[pt : pt + 1, k : k + 1], (1, lanes))
            mix_own[2 * pt + k : 2 * pt + k + 1, :] = (2.0 * level.astype(jnp.float32) - 7.0) / 7.0
    mix_all[pl.ds(g, 1)] = mix_own[...][None]

    def mix_copy(d):
        return pltpu.make_async_remote_copy(
            src_ref=mix_own, dst_ref=mix_all.at[g],
            send_sem=mix_send, recv_sem=mix_recv,
            device_id=(lax.rem(g + d, n_grid), f), device_id_type=MESH,
        )

    for d in range(1, n_grid):
        pl.semaphore_signal(
            known_sem, inc=1, device_id=(lax.rem(g + d, n_grid), f), device_id_type=MESH
        )
        mix_copy(d).start()

    acc[...] = jnp.zeros_like(acc)

    sign = jnp.where(2 * z < nz, 1, -1)

    def take_in(p):
        for d in range(1, nz):
            s = lax.rem(z + nz + sign * d, nz)
            chain_copy(p, s, z).wait_recv()

            @pl.when(jnp.logical_and(jnp.logical_and(s < z, s > 0), z < last))
            def _():
                chain_copy(p, s, z + 1).start()

            @pl.when(jnp.logical_and(jnp.logical_and(s > z, s < last), z > 0))
            def _():
                chain_copy(p, s, z - 1).start()

            pair_copy(p, s).start()

    def compute(p):
        pltpu.make_async_remote_copy(
            src_ref=x_buf.at[p, 1 - core], dst_ref=x_buf.at[p, 1 - core],
            send_sem=pair_send, recv_sem=pair_recv.at[p],
            device_id=(g, f + 1 - 2 * core), device_id_type=MESH,
        ).wait_recv()
        pltpu.make_async_copy(w_buf.at[p], w_buf.at[p], w_sem.at[p]).wait()
        x = x_buf[p].reshape(lanes, kp)
        for j in range(3):
            acc[j] += lax.dot_general(
                w_buf[p, j], x, (((1,), (1,)), ((), ())),
                preferred_element_type=jnp.float32,
            )

    @pl.loop(0, NUM_PIECES)
    def _(p):
        take_in(p)

        @pl.when(p > 0)
        def _():
            compute(p - 1)

    compute(NUM_PIECES - 1)

    pltpu.make_async_copy(
        mix_all.at[: n_grid - 1], mix_all.at[: n_grid - 1], mix_recv
    ).wait()
    small[3].wait()

    n_pts = n_grid * pts
    coef = []
    for pt in range(n_pts):
        r = 2 * (pt % pts)
        coef.append([mix_all[pt // pts, r + k : r + k + 1, :] for k in range(2)])
    scaled = [[jnp.broadcast_to(LOG2E * v, (8, lanes)) for v in pair] for pair in coef]

    lane_chunk = lax.rem(lax.broadcasted_iota(jnp.int32, (8, lanes), 1) // chunk, nz)
    targets = jnp.zeros((8, lanes), jnp.int32)
    for s in range(nz):
        row = jnp.broadcast_to(targets_ref[s : s + 1, :], (8, lanes))
        row = pltpu.roll(row, lax.rem((s - g) * chunk + lanes, lanes), 1)
        targets = jnp.where(lane_chunk == s, row, targets)
    targets = targets - f * vocab

    tall = ROW_CHUNK // 8
    sub = lax.broadcasted_iota(jnp.int32, (tall, 8, lanes), 0) * 8 + lax.broadcasted_iota(
        jnp.int32, (tall, 8, lanes), 1
    )

    def step(c, carry):
        tops, sums, picks = carry
        at = pl.ds(pl.multiple_of(c * ROW_CHUNK, ROW_CHUNK), ROW_CHUNK)
        parts = [acc[j, at, :].reshape(tall, 8, lanes) for j in range(3)]
        hit = sub == (targets - c * ROW_CHUNK)[None]
        picks = tuple(
            pk + jnp.sum(jnp.where(hit, part, 0.0), axis=0) for pk, part in zip(picks, parts)
        )
        centre = LOG2E * parts[0]
        new_tops, new_sums = [], []
        for pt in range(n_pts):
            logit = centre + scaled[pt][0][None] * parts[1] + scaled[pt][1][None] * parts[2]
            top = jnp.maximum(tops[pt], jnp.max(logit, axis=0))
            new_sums.append(
                sums[pt] * jnp.exp2(tops[pt] - top)
                + jnp.sum(jnp.exp2(logit - top[None]), axis=0)
            )
            new_tops.append(top)
        return tuple(new_tops), tuple(new_sums), picks

    low = jnp.full((8, lanes), -jnp.inf, jnp.float32)
    zero = jnp.zeros((8, lanes), jnp.float32)
    tops, sums, picks = lax.fori_loop(
        0, vocab // ROW_CHUNK, step, ((low,) * n_pts, (zero,) * n_pts, (zero,) * 3)
    )
    picks = [jnp.sum(pk, axis=0, keepdims=True) for pk in picks]
    for pt in range(n_pts):
        at, row = pt // pts, pt % pts
        top = jnp.max(tops[pt], axis=0, keepdims=True)
        total = jnp.sum(sums[pt] * jnp.exp2(tops[pt] - top), axis=0, keepdims=True)
        stat_own[at, row : row + 1, :] = LN2 * top + jnp.log(total)
        stat_own[at, pts + row : pts + row + 1, :] = (
            picks[0] + coef[pt][0] * picks[1] + coef[pt][1] * picks[2]
        )
    stat_all[pl.ds(me, 1)] = stat_own[pl.ds(g, 1)]

    pltpu.make_async_copy(
        x_buf.at[:, 0, :last], x_buf.at[:, 0, :last], chain_send
    ).wait()
    pltpu.make_async_copy(x_buf.at[:, 0], x_buf.at[:, 0], pair_send).wait()
    pltpu.make_async_copy(
        mix_all.at[: n_grid - 1], mix_all.at[: n_grid - 1], mix_send
    ).wait()
    pl.semaphore_wait(known_sem, n_grid - 1)

    @pl.loop(1, n_all)
    def _(d):
        to = lax.rem(me + d, n_all)
        tg, tf = to // n_fsdp, lax.rem(to, n_fsdp)
        pltpu.make_async_remote_copy(
            src_ref=stat_own.at[tg], dst_ref=stat_all.at[me],
            send_sem=stat_send, recv_sem=stat_recv,
            device_id=(tg, tf), device_id_type=MESH,
        ).start()

    others = stat_all.at[: n_all - 1]
    pltpu.make_async_copy(others, others, stat_recv).wait()

    everything = jnp.zeros((pts, lanes), jnp.float32)
    chosen = jnp.zeros((pts, lanes), jnp.float32)
    lane = lax.broadcasted_iota(jnp.int32, (pts, lanes), 1)
    start = core * nz * chunk + z * chunk
    for column in range(n_grid):
        here = stat_all[column * n_fsdp : (column + 1) * n_fsdp]
        lse = here[:, :pts]
        top = jnp.max(lse, axis=0)
        loss = top + jnp.log(jnp.sum(jnp.exp(lse - top[None]), axis=0))
        loss = loss - jnp.sum(here[:, pts:], axis=0)
        everything = everything + loss
        moved = pltpu.roll(loss, lax.rem(column * chunk + lanes - start, lanes), 1)
        chosen = jnp.where(lane // chunk == column, moved, chosen)
    packed_ref[:pts, :] = chosen
    for pt in range(pts):
        mean = jnp.sum(everything[pt : pt + 1, :], axis=1, keepdims=True) / total_tokens
        packed_ref[pts + pt : pts + pt + 1, :] = jnp.broadcast_to(mean, (1, lanes))

    pltpu.make_async_copy(others, others, stat_send).wait()


def split(packed_ref, token_ref, mean_ref):
    pts, own = token_ref.shape
    token_ref[...] = packed_ref[:pts, :own]
    for pt in range(pts):
        mean_ref[pt] = packed_ref[pts + pt, 0]


def body(n_grid, n_fsdp, hidden, norm_gain, base_head, first_dir, second_dir, coords, targets):
    own, width = hidden.shape
    vocab = base_head.shape[0]
    pts = coords.shape[0]
    total = targets.shape[0]
    nz = n_fsdp // 2
    chunk = own // n_grid
    lanes = 2 * nz * chunk
    assert nz == n_grid and own == nz * chunk and total == n_grid * lanes
    kp = width // NUM_PIECES
    n_all = n_grid * n_fsdp
    dma = pltpu.SemaphoreType.DMA
    vmem = pl.BlockSpec(memory_space=pltpu.VMEM)
    smem = pl.BlockSpec(memory_space=pltpu.SMEM)
    anywhere = pl.BlockSpec(memory_space=pl.ANY)
    packed = pl.pallas_call(
        functools.partial(kernel, n_grid, n_fsdp, total),
        out_shape=jax.ShapeDtypeStruct((2 * pts, lanes), jnp.float32),
        in_specs=[anywhere] * 7,
        out_specs=vmem,
        scratch_shapes=[
            pltpu.VMEM((pts, 2), jnp.int32),
            pltpu.VMEM((chunk, width), jnp.bfloat16),
            pltpu.VMEM((1, width), jnp.float32),
            pltpu.VMEM((nz, 2 * own), jnp.int32),
            pltpu.VMEM((NUM_PIECES, 3, vocab, kp), jnp.bfloat16),
            pltpu.VMEM((NUM_PIECES, 2, nz, chunk, kp), jnp.bfloat16),
            pltpu.VMEM((3, vocab, lanes), jnp.float32),
            pltpu.VMEM((2 * pts, lanes), jnp.float32),
            pltpu.VMEM((n_grid, 2 * pts, lanes), jnp.float32),
            pltpu.VMEM((n_grid, 2 * pts, lanes), jnp.float32),
            pltpu.VMEM((n_all, 2 * pts, lanes), jnp.float32),
            dma((4,)),
            dma((NUM_PIECES,)),
            dma,
            dma((NUM_PIECES, nz)),
            dma,
            dma((NUM_PIECES,)),
            dma,
            dma,
            dma,
            dma,
            pltpu.SemaphoreType.REGULAR,
        ],
        compiler_params=pltpu.CompilerParams(
            collective_id=0, has_side_effects=True, vmem_limit_bytes=60 * 1024 * 1024
        ),
    )(
        coords, hidden, norm_gain.reshape(1, width), targets.reshape(nz, 2 * own),
        base_head, first_dir, second_dir,
    )
    return tuple(
        pl.pallas_call(
            split,
            out_shape=(
                jax.ShapeDtypeStruct((pts, own), jnp.float32),
                jax.ShapeDtypeStruct((pts,), jnp.float32),
            ),
            in_specs=[vmem],
            out_specs=(vmem, smem),
        )(packed)
    )


def solution(mesh):
    placed = (
        P("fsdp", None),
        P(),
        P("fsdp", None),
        P("fsdp", None),
        P("fsdp", None),
        P("grid", None),
        P(),
    )
    n_grid, n_fsdp = mesh.shape["grid"], mesh.shape["fsdp"]
    return jax.shard_map(
        functools.partial(body, n_grid, n_fsdp),
        mesh=mesh, in_specs=placed, out_specs=(P("grid", "fsdp"), P("grid")), check_vma=False,
    )
```
